128 devices in a mesh: dp: 16 (over y, x), mp: 8 (over z, core).
Axes of the slice: x: 4, y: 4, z: 4, core: 2. Of those that a mesh axis runs over, the one named last changes fastest.
Arguments:
- tokens: bfloat16 [65536, 1024], P(('dp', 'mp')), may hold values from -6 to 6
- norm_gain: float32 [2, 1024], replicated, may hold values from 0.1 to 1.9
- qkv_weight: bfloat16 [3, 1024, 1024], P(None, 'dp', 'mp')
- out_weight: bfloat16 [1024, 1024], P('mp', 'dp'), may hold values from -0.1875 to 0.1875
- variate_bias: float32 [2, 16], replicated, may hold values from -6 to 6
- ffn_weight: bfloat16 [2, 1024, 2816], P(None, 'dp', 'mp'), may hold values from -0.1875 to 0.1875
- down_weight: bfloat16 [2816, 1024], P('mp', 'dp'), may hold values from -0.109375 to 0.109375
- sample_ids: int32 [65536], P(('dp', 'mp')), may hold values from 0 to 127, as said below
- variate_ids: int32 [65536], P(('dp', 'mp')), may hold values from 0 to 15, as said below
- time_ids: int32 [65536], P(('dp', 'mp')), may hold values from 0 to 31, as said below
Outputs:
- encoded: bfloat16 [65536, 1024], P(('dp', 'mp'))
The draws below stay inside these ranges and needn't reach their ends.
Inputs may be any that keep to these rules, and one draw needn't show every extreme that they name: `sample_ids`: within each packed sequence of 512 tokens the series numbers start at 0 and never fall; a series with v variates (1 to 16) and p patches (4 to 32) holds v * p consecutive tokens, the last series of a sequence may be cut short; some packed sequence holds 128 series of one variate and four patches each. `variate_ids`: A token's offset within its series divided by that series' patch count p. `time_ids`: A token's offset within its series modulo that series' patch count p.
All inputs are finite; a program needn't handle non-finite values.
Results may differ from the reference program's by a relative error of at most 0.017.
Values may be sent and summed in bfloat16 or wider, within the bound.
A program may use at most 128 MiB of HBM per device.

```python
import jax
import jax.numpy as jnp
from jax import lax

D = 1024
HEAD_DIM = 64
HEADS = 16
FF = 2816
L = 512
SEQS = 128
TOKENS = 65536


def packing(key):
    key_var, key_pat, key_pick = jax.random.split(jax.random.fold_in(key, 5), 3)
    slots = L // 4
    variates = jax.random.randint(key_var, (SEQS, slots), 1, 17)
    patches = jax.random.randint(key_pat, (SEQS, slots), 4, 33)
    chosen = jax.random.randint(key_pick, (), 0, SEQS)
    dense = (jnp.arange(SEQS, dtype=jnp.int32) == chosen)[:, None]
    variates = jnp.where(dense, 1, variates)
    patches = jnp.where(dense, 4, patches)
    lengths = variates * patches
    ends = jnp.cumsum(lengths, axis=1)
    starts = ends - lengths
    position = jnp.arange(L, dtype=jnp.int32)
    series = jnp.sum((position[None, :, None] >= ends[:, None, :]).astype(jnp.int32), axis=2)
    begin = jnp.take_along_axis(starts, series, axis=1)
    span = jnp.take_along_axis(patches, series, axis=1)
    offset = position[None, :] - begin
    return (series.reshape(-1).astype(jnp.int32), (offset // span).reshape(-1).astype(jnp.int32), (offset % span).reshape(-1).astype(jnp.int32))


def draw_sample_ids(key, part):
    return packing(key)[0]


def draw_variate_ids(key, part):
    return packing(key)[1]


def draw_time_ids(key, part):
    return packing(key)[2]


def draw_qkv_weight(key, part):
    key_base = jax.random.fold_in(jax.random.fold_in(key, 11), 0)
    base = jax.random.normal(key_base, (3, D, D), jnp.float32) * D ** (-0.5)
    return base.astype(jnp.bfloat16)


def shard_levels(stream_key, extent, shards, least, top_value):
    level, own = 1.0, jax.random.fold_in(stream_key, 6)
    for dim, shards_of in shards:
        heights = jnp.exp(jax.random.uniform(jax.random.fold_in(own, dim), (shards_of,), jnp.float32, least / len(shards), top_value / len(shards)))
        level = level * jnp.repeat(heights, extent[dim] // shards_of).reshape([-1 if axis == dim else 1 for axis in range(len(extent))])
    return level


def gaussian(stream_key, dims, spread, most, pieces=(), held_as=jnp.bfloat16):
    level = shard_levels(stream_key, dims, pieces, -0.22, 0.18) if pieces else 1.0
    entries = jax.random.normal(stream_key, dims, jnp.float32) * spread * level
    return jnp.minimum(jnp.maximum(entries, -most), most).astype(held_as)


def setup_inputs(seed: int = 0) -> dict:
    keys = jax.random.split(jax.random.key(seed), 11)
    tokens = gaussian(keys[0], (TOKENS, D), 1.0, 6.0, ((0, 128),))
    norm_gain = jnp.clip(1.0 + 0.18 * jax.random.normal(keys[1], (2, D), jnp.float32), 0.1, 1.9)
    qkv_weight = draw_qkv_weight(jax.random.fold_in(keys[10], 71), 0)
    out_weight = gaussian(keys[3], (D, D), D ** -0.5, 0.1875, ((0, 8), (1, 16)))
    variate_bias = gaussian(keys[4], (2, HEADS), 1.5, 6.0, (), jnp.float32)
    ffn_weight = gaussian(keys[5], (2, D, FF), D ** -0.5, 0.1875, ((1, 16), (2, 8)))
    down_weight = gaussian(keys[6], (FF, D), FF ** -0.5, 0.109375, ((0, 8), (1, 16)))
    sample_ids = draw_sample_ids(jax.random.fold_in(keys[10], 71), 0)
    variate_ids = draw_variate_ids(jax.random.fold_in(keys[10], 71), 0)
    time_ids = draw_time_ids(jax.random.fold_in(keys[10], 71), 0)
    return dict(tokens=tokens, norm_gain=norm_gain, qkv_weight=qkv_weight, out_weight=out_weight, variate_bias=variate_bias, ffn_weight=ffn_weight, down_weight=down_weight, sample_ids=sample_ids, variate_ids=variate_ids, time_ids=time_ids)


def rms_norm(values, gain):
    wide = values.astype(jnp.float32)
    square = lax.optimization_barrier(jnp.mean(wide * wide, axis=-1, keepdims=True))
    return (wide * lax.rsqrt(square + 1e-05) * gain[None, :]).astype(jnp.bfloat16)

def rotate(values, times):
    half = values.shape[-1] // 2
    freq = 10000.0 ** (-jnp.arange(half, dtype=jnp.float32) / half)
    angle = times.astype(jnp.float32)[:, None] * freq[None, :]
    cosine = jnp.cos(angle)[:, None, :]
    sine = jnp.sin(angle)[:, None, :]
    first = values[..., :half]
    second = values[..., half:]
    return jnp.concatenate([first * cosine - second * sine, first * sine + second * cosine], axis=-1)

def reference(tokens, norm_gain, qkv_weight, out_weight, variate_bias, ffn_weight, down_weight, sample_ids, variate_ids, time_ids):
    total = tokens.shape[0]
    first_normed = rms_norm(tokens, norm_gain[0])
    query_raw = jnp.dot(first_normed, qkv_weight[0], preferred_element_type=jnp.float32)
    key_raw = jnp.dot(first_normed, qkv_weight[1], preferred_element_type=jnp.float32)
    value_raw = jnp.dot(first_normed, qkv_weight[2], preferred_element_type=jnp.float32)
    queries = rotate(query_raw.reshape(total, HEADS, HEAD_DIM), time_ids).astype(jnp.bfloat16)
    keys_rot = rotate(key_raw.reshape(total, HEADS, HEAD_DIM), time_ids).astype(jnp.bfloat16)
    values = value_raw.reshape(total, HEADS, HEAD_DIM).astype(jnp.bfloat16)
    count = total // L

    def one_sequence(args):
        qs, ks, vs, samples, variates = args
        scores = jnp.einsum('qhd,khd->hqk', qs.astype(jnp.float32), ks.astype(jnp.float32)) * HEAD_DIM ** (-0.5)
        same = variates[:, None] == variates[None, :]
        scores = scores + jnp.where(same[None], variate_bias[0][:, None, None], variate_bias[1][:, None, None])
        scores = jnp.where((samples[:, None] == samples[None, :])[None], scores, -1e+30)
        top = lax.optimization_barrier(jnp.max(scores, axis=2, keepdims=True))
        expo = jnp.exp(scores - top)
        weights = (expo / lax.optimization_barrier(jnp.sum(expo, axis=2, keepdims=True))).astype(jnp.bfloat16)
        return jnp.einsum('hqk,khd->qhd', weights.astype(jnp.float32), vs.astype(jnp.float32)).astype(jnp.bfloat16)
    attended = lax.map(one_sequence, (queries.reshape(count, L, HEADS, HEAD_DIM), keys_rot.reshape(count, L, HEADS, HEAD_DIM), values.reshape(count, L, HEADS, HEAD_DIM), sample_ids.reshape(count, L), variate_ids.reshape(count, L)))
    attended = attended.reshape(total, D)
    residual = (tokens.astype(jnp.float32) + jnp.dot(attended, out_weight, preferred_element_type=jnp.float32)).astype(jnp.bfloat16)
    second_normed = rms_norm(residual, norm_gain[1])
    gate = jnp.dot(second_normed, ffn_weight[0], preferred_element_type=jnp.float32)
    up = jnp.dot(second_normed, ffn_weight[1], preferred_element_type=jnp.float32)
    hidden = (jax.nn.silu(gate) * up).astype(jnp.bfloat16)
    return (residual.astype(jnp.float32) + jnp.dot(hidden, down_weight, preferred_element_type=jnp.float32)).astype(jnp.bfloat16)
```

```python
import jax
import jax.numpy as jnp
from jax import lax
from jax.sharding import PartitionSpec as P

HEAD_DIM = 64
L = 512


def sent_to_all(shard, axis):
    copies = jnp.broadcast_to(shard, (lax.axis_size(axis), *shard.shape))
    return lax.all_to_all(copies, axis, split_axis=0, concat_axis=0, tiled=True)


def in_order(blocks, dim):
    blocks = jnp.moveaxis(blocks, 0, dim)
    dims = blocks.shape
    return blocks.reshape(*dims[:dim], dims[dim] * dims[dim + 1], *dims[dim + 2 :])


def collect(shard, axis, dim):
    blocks = sent_to_all(shard, axis)
    return in_order(blocks, dim)


def rows_first(arrays, axis, dims):
    turned = [jnp.moveaxis(a, dim, 0) for a, dim in zip(arrays, dims)]
    widths = [t[0].size for t in turned]
    both = jnp.concatenate([t.reshape(-1, w) for t, w in zip(turned, widths)], axis=1)
    whole = lax.all_gather(both, axis, axis=0, tiled=True)
    blocks = jnp.split(whole, [sum(widths[:k]) for k in range(1, len(widths))], axis=1)
    return tuple(
        (
            jnp.moveaxis(b.reshape(-1, *t.shape[1:]), 0, dim)
            for b, t, dim in zip(blocks, turned, dims)
        )
    )


def rms_norm(values, gain):
    wide = values.astype(jnp.float32)
    square = jnp.mean(wide * wide, axis=-1, keepdims=True)
    return (wide * lax.rsqrt(square + 1e-05) * gain[None, :]).astype(jnp.bfloat16)


def rotate(values, times):
    half = values.shape[-1] // 2
    freq = 10000.0 ** (-jnp.arange(half, dtype=jnp.float32) / half)
    angle = times.astype(jnp.float32)[:, None] * freq[None, :]
    cosine = jnp.cos(angle)[:, None, :]
    sine = jnp.sin(angle)[:, None, :]
    first = values[..., :half]
    second = values[..., half:]
    return jnp.concatenate(
        [first * cosine - second * sine, first * sine + second * cosine], axis=-1
    )


def rotated(raw, times):
    row_total, local_width = raw.shape
    turned = rotate(raw.reshape(row_total, local_width // HEAD_DIM, HEAD_DIM), times)
    return turned.reshape(row_total, local_width).astype(jnp.bfloat16)


def attend(queries, keys_rot, values, samples, variates, bias):
    row_total, local_width = queries.shape
    heads_here = local_width // HEAD_DIM
    count = row_total // L

    def one_sequence(args):
        qs, ks, vs, sample_row, variate_row = args
        scores = jnp.einsum(
            "qhd,khd->hqk", qs, ks, preferred_element_type=jnp.float32
        ) * HEAD_DIM ** (-0.5)
        same = variate_row[:, None] == variate_row[None, :]
        scores = scores + jnp.where(same[None], bias[0][:, None, None], bias[1][:, None, None])
        scores = jnp.where((sample_row[:, None] == sample_row[None, :])[None], scores, -1e30)
        top = jnp.max(scores, axis=2, keepdims=True)
        expo = jnp.exp(scores - top)
        weights = (expo / jnp.sum(expo, axis=2, keepdims=True)).astype(jnp.bfloat16)
        return jnp.einsum("hqk,khd->qhd", weights, vs, preferred_element_type=jnp.float32).astype(
            jnp.bfloat16
        )

    shape = (count, L, heads_here, HEAD_DIM)
    result = lax.map(
        one_sequence,
        (
            queries.reshape(shape),
            keys_rot.reshape(shape),
            values.reshape(shape),
            samples.reshape(count, L),
            variates.reshape(count, L),
        ),
    )
    return result.reshape(row_total, local_width)


def gathered(shard):
    return lax.all_gather(shard, ("dp", "mp"), axis=0, tiled=False)


def local(
    tokens,
    norm_gain,
    qkv_weight,
    out_weight,
    variate_bias,
    ffn_weight,
    down_weight,
    sample_ids,
    variate_ids,
    time_ids,
):
    first_normed = rms_norm(tokens, norm_gain[0])
    qkv = gathered(qkv_weight).reshape(16, 8, 3, 64, 128)
    qkv = qkv.transpose(2, 0, 3, 1, 4).reshape(3, 1024, 1024)
    projected = jnp.einsum("rc,jcd->jrd", first_normed, qkv, preferred_element_type=jnp.float32)
    queries = rotated(projected[0], time_ids)
    keys_rot = rotated(projected[1], time_ids)
    values = projected[2].astype(jnp.bfloat16)
    attended = attend(queries, keys_rot, values, sample_ids, variate_ids, variate_bias)
    out_full = gathered(out_weight.T).reshape(16, 8, 64, 128).transpose(0, 2, 1, 3).reshape(1024, 1024)
    mixed = jnp.einsum("rc,dc->rd", attended, out_full, preferred_element_type=jnp.float32)
    residual = (tokens.astype(jnp.float32) + mixed).astype(jnp.bfloat16)
    second_normed = rms_norm(residual, norm_gain[1])
    ffn = gathered(ffn_weight).reshape(16, 8, 2, 64, 352)
    ffn = ffn.transpose(2, 0, 3, 1, 4).reshape(2, 1024, 2816)
    gate_up = jnp.einsum("rc,jcf->jrf", second_normed, ffn, preferred_element_type=jnp.float32)
    hidden = (jax.nn.silu(gate_up[0]) * gate_up[1]).astype(jnp.bfloat16)
    down = gathered(down_weight.T).reshape(16, 8, 64, 352).transpose(0, 2, 1, 3).reshape(1024, 2816)
    feed = jnp.einsum("rf,df->rd", hidden, down, preferred_element_type=jnp.float32)
    return (residual.astype(jnp.float32) + feed).astype(jnp.bfloat16)


def solution(mesh):
    return jax.shard_map(
        local,
        mesh=mesh,
        in_specs=(
            P(("dp", "mp"), None),
            P(),
            P(None, "dp", "mp"),
            P("mp", "dp"),
            P(),
            P(None, "dp", "mp"),
            P("mp", "dp"),
            P(("dp", "mp")),
            P(("dp", "mp")),
            P(("dp", "mp")),
        ),
        out_specs=P(("dp", "mp"), None),
        check_vma=False,
    )
```

```python
import functools

import jax
import jax.numpy as jnp
import numpy as np
from jax import lax
from jax.experimental import pallas as pl
from jax.experimental.pallas import tpu as pltpu
from jax.sharding import PartitionSpec as P

L = 512
D = 1024
TIMES = 32
LOG2E = 1.4426950408889634
BF = jnp.bfloat16
F32 = jnp.float32
MESH = pl.DeviceIdType.MESH

A, B, C = 0, 1, 2
ORDERS = (("x", "y", "z"), ("y", "z", "x"), ("z", "x", "y"))
OUT_ROWS = (32, 16, 16)
OUT_AT = (0, 32, 48)
ROWS = ((64, 64, 64), tuple(128 + r for r in OUT_ROWS), (64, 64, 64))
HALF = ((32, 32, 32), (80, 80, 80), (32, 32, 32))
B_AT = (0, 160, 304)
OWN = 24


class Exchange:
    def __init__(self, bufs, send, recv):
        self.bufs, self.send, self.recv = bufs, send, recv
        dp, mp = lax.axis_index("dp"), lax.axis_index("mp")
        self.pos = {"x": lax.rem(dp, 4), "y": dp // 4, "z": mp // 2}
        self.core = lax.rem(mp, 2)
        self.started = []

    def device(self, axis=None, step=0):
        pos = dict(self.pos)
        core = self.core
        if axis == "core":
            core = 1 - core
        elif axis is not None:
            pos[axis] = lax.rem(pos[axis] + step + 4, 4)
        return (pos["y"] * 4 + pos["x"], pos["z"] * 2 + core)

    def slab(self, b, c, phase, shift, half):
        a1, a2, a3 = ORDERS[c]
        at = {k: self.pos[k] for k in "xyz"}
        axis = ORDERS[c][phase]
        at[axis] = lax.rem(at[axis] + shift + 4, 4)
        buf = self.bufs[b][c]
        base = self.core * 64 + at[a3] * 16
        if phase == 0:
            first = base + at[a2] * 4 + at[a1]
            top = HALF[b][c]
            rows = pl.ds(0, top) if half == 0 else pl.ds(top, ROWS[b][c] - top)
            return buf.at[pl.ds(first, 1), rows]
        if phase == 1:
            return buf.at[pl.ds(base + at[a2] * 4 + 2 * half, 2)]
        return buf.at[pl.ds(base + 8 * half, 8)]

    def copy(self, ref, b, c, slot, device):
        return pltpu.make_async_remote_copy(
            src_ref=ref,
            dst_ref=ref,
            send_sem=self.send.at[b, c, slot],
            recv_sem=self.recv.at[b, c, slot],
            device_id=device,
            device_id_type=MESH,
        )

    def start(self, b, c, slot, ref, device):
        copy = self.copy(ref, b, c, slot, device)
        copy.start()
        self.started.append(copy)

    def first(self, b, c, p):
        axis = ORDERS[c][p]
        for slot, half, step in ((0, 0, 1), (2, 1, -1), (1, 1, 1), (3, 0, -1)):
            self.start(b, c, p * 6 + slot, self.slab(b, c, p, 0, half), self.device(axis, step))

    def landed(self, b, c, p, slot):
        half = (0, 1, 1, 0, 0, 1)[slot]
        shift = (-1, -1, 1, 1, -2, 2)[slot]
        ref = self.slab(b, c, p, shift, half)
        self.copy(ref, b, c, p * 6 + slot, self.device(ORDERS[c][p], 1)).wait_recv()
        return ref

    def forward(self, b, c, p):
        axis = ORDERS[c][p]
        for slot, step in ((0, 1), (2, -1)):
            ref = self.landed(b, c, p, slot)
            self.start(b, c, p * 6 + 4 + slot // 2, ref, self.device(axis, step))
            if p == 2:
                self.share(b, c, slot, ref)

    def finish(self, b, c, p, slots=(1, 3, 4, 5)):
        for slot in slots:
            ref = self.landed(b, c, p, slot)
            if p == 2:
                self.share(b, c, slot, ref)

    def share(self, b, c, slot, ref):
        self.start(b, c, 18 + slot, ref, self.device("core"))

    def plane(self, b, c, core):
        return self.bufs[b][c].at[pl.ds(core * 64 + self.pos[ORDERS[c][2]] * 16, 16)]

    def share_own(self, b, c):
        self.start(b, c, OWN, self.plane(b, c, self.core), self.device("core"))

    def shared(self, b, c):
        other = self.device("core")
        self.copy(self.plane(b, c, self.core), b, c, OWN, other).wait_recv()
        for slot in range(6):
            ref = self.slab(b, c, 2, (-1, -1, 1, 1, -2, 2)[slot], (0, 1, 1, 0, 0, 1)[slot])
            self.copy(ref, b, c, 18 + slot, other).wait_recv()

    def every(self, action, b, p):
        for c in range(3):
            action(b, c, p)


def nt(a, b):
    return lax.dot_general(a, b, (((1,), (1,)), ((), ())), preferred_element_type=F32)


def nn(a, b):
    return jnp.dot(a, b, preferred_element_type=F32)


def spot(c, core, x, y, z):
    at = {"x": x, "y": y, "z": z}
    a1, a2, a3 = ORDERS[c]
    return core * 64 + at[a3] * 16 + at[a2] * 4 + at[a1]


def normed_into(dst, src, gain, row):
    g = gain[pl.ds(row, 1), :]

    def block(i, _):
        rows = pl.ds(pl.multiple_of(i * 64, 64), 64)
        wide = src[rows, :].astype(F32)
        square = jnp.mean(wide * wide, axis=-1, keepdims=True)
        dst[rows, :] = (wide * lax.rsqrt(square + 1e-05) * g).astype(BF)
        return 0

    lax.fori_loop(0, 8, block, 0)


def kernel(
    tok, gain, qkvw, packb, packc, table, slope, sids, vids, tids,
    out,
    a0, a1, a2, b0, b1, b2, c0, c1, c2,
    xn, same, away, cq, sq, ck, sk, qs, ks, vs, att, res, hid,
    stage, send, recv,
):
    ex = Exchange(((a0, a1, a2), (b0, b1, b2), (c0, c1, c2)), send, recv)

    def source(b, c):
        if b == A:
            return qkvw.at[c]
        if b == B:
            return packb.at[pl.ds(B_AT[c], ROWS[B][c])]
        return packc.at[c]

    def own(b, c):
        first = spot(c, ex.core, ex.pos["x"], ex.pos["y"], ex.pos["z"])
        return pltpu.make_async_copy(source(b, c), ex.bufs[b][c].at[first], stage.at[b, c])

    for b in (A, B, C):
        for c in range(3):
            own(b, c).start()
    barrier = pltpu.get_barrier_semaphore()
    for axis in "xyz":
        for step in (1, -1):
            pl.semaphore_signal(barrier, inc=1, device_id=ex.device(axis, step), device_id_type=MESH)
    pl.semaphore_signal(barrier, inc=1, device_id=ex.device("core"), device_id_type=MESH)
    pl.semaphore_wait(barrier, 7)

    for b in (A, B, C):
        for c in range(3):
            own(b, c).wait()
        ex.every(ex.first, b, 0)

    normed_into(xn, tok, gain, 0)
    for b in (A, B, C):
        ex.every(ex.forward, b, 0)

    eye = (
        lax.broadcasted_iota(jnp.int32, (L, L), 0) == lax.broadcasted_iota(jnp.int32, (L, L), 1)
    ).astype(F32).astype(BF)

    def column(ids):
        row = jnp.broadcast_to(ids[...].astype(F32), (128, L)).astype(BF)
        return nt(eye, row)

    def matches(ids):
        col = column(ids)
        row = jnp.broadcast_to(ids[...].astype(F32), (L, L))
        return jnp.concatenate([col] * 4, axis=1) == row

    same[...] = jnp.where(matches(vids), 1.0, 0.0)
    away[...] = jnp.where(matches(sids), 0.0, -1e30)

    ex.every(ex.finish, A, 0)
    ex.every(ex.first, A, 1)
    ex.every(ex.finish, C, 0)
    ex.every(ex.first, C, 1)

    lanes = lax.broadcasted_iota(jnp.int32, (L, 128), 1).astype(F32)
    hot = jnp.where(column(tids) == lanes, 1.0, 0.0).astype(BF)
    turn = nn(hot, table[...])
    cos = turn[:, 0:128] + turn[:, 256:384] + turn[:, 512:640]
    sin = turn[:, 128:256] + turn[:, 384:512] + turn[:, 640:768]
    cq[...] = cos * (LOG2E / 8.0)
    sq[...] = sin * (LOG2E / 8.0)
    ck[...] = cos
    sk[...] = sin

    ex.every(ex.forward, A, 1)
    ex.every(ex.finish, B, 0)
    ex.every(ex.finish, A, 1)
    ex.every(ex.first, A, 2)
    for c in range(3):
        ex.share_own(A, c)
    ex.every(ex.first, B, 1)
    ex.every(ex.forward, C, 1)
    ex.every(ex.finish, C, 1)
    ex.every(ex.forward, A, 2)
    ex.every(ex.forward, B, 1)
    ex.every(ex.finish, B, 1)
    ex.every(ex.first, B, 2)
    for c in range(3):
        ex.share_own(B, c)
    for c in range(3):
        ex.share_own(C, c)
    ex.every(ex.finish, A, 2)
    for c in range(3):
        ex.shared(A, c)

    def columns(b, c, z, rows):
        sides = []
        for core in range(2):
            parts = [
                ex.bufs[b][c][spot(c, core, x, y, z), rows, :]
                for y in range(4)
                for x in range(4)
            ]
            sides.append(jnp.concatenate(parts, axis=0))
        return jnp.concatenate(sides, axis=1)

    def turned(raw, cosine, sine):
        lane = lax.rem(lax.broadcasted_iota(jnp.int32, (L, 128), 1), 64)
        done = []
        for t in range(2):
            v = raw[:, t * 128 : (t + 1) * 128]
            other = jnp.where(lane < 32, pltpu.roll(v, 96, 1), pltpu.roll(v, 32, 1))
            done.append(v * cosine[...] + other * sine[...])
        return jnp.concatenate(done, axis=1).astype(BF)

    def group(z):
        every = slice(0, 64)
        qs[...] = turned(nn(xn[...], columns(A, 0, z, every)), cq, sq)
        ks[...] = turned(nn(xn[...], columns(A, 1, z, every)), ck, sk)
        vs[...] = nn(xn[...], columns(A, 2, z, every)).astype(BF)

        def head(h, _):
            mine = lax.broadcasted_iota(jnp.int32, (L, 256), 1) // 64 == h
            q = jnp.where(mine, qs[...], jnp.zeros((), BF))
            s = nt(q, ks[...]) + same[...] * slope[z * 4 + h] + away[...]
            e = jnp.exp2(s - jnp.max(s, axis=1, keepdims=True))
            total = jnp.sum(e, axis=1, keepdims=True)
            got = (nn(e.astype(BF), vs[...]) * (1.0 / total)).astype(BF)
            here = pl.ds(z * 256, 256)
            att[:, here] = jnp.where(mine, got, att[:, here])
            return 0

        lax.fori_loop(0, 4, head, 0)

    att[...] = jnp.zeros_like(att)
    group(0)
    group(1)
    ex.every(ex.forward, B, 2)
    ex.every(ex.first, C, 2)
    group(2)
    group(3)
    ex.every(functools.partial(ex.finish, slots=(1, 3)), B, 2)

    def project(y, _):
        tall = []
        for z in range(4):
            for core in range(2):
                parts = [
                    ex.bufs[B][c][spot(c, core, x, y, z), 0 : OUT_ROWS[c], :]
                    for x in range(4)
                    for c in range(3)
                ]
                tall.append(jnp.concatenate(parts, axis=0))
        here = pl.ds(pl.multiple_of(y * 256, 256), 256)
        mixed = nt(att[...], jnp.concatenate(tall, axis=1))
        res[:, here] = (tok[:, here].astype(F32) + mixed).astype(BF)
        return 0

    ex.every(functools.partial(ex.finish, slots=(4, 5)), B, 2)
    for c in range(3):
        ex.shared(B, c)
    lax.fori_loop(0, 4, project, 0)
    normed_into(xn, res, gain, 1)

    def feed(z, _):
        for c in range(3):
            r = OUT_ROWS[c]
            gate = nn(xn[...], columns(B, c, z, slice(r, r + 64)))
            up = nn(xn[...], columns(B, c, z, slice(r + 64, r + 128)))
            wide = gate / (1.0 + jnp.exp(-gate)) * up
            hid[:, pl.ds(pl.multiple_of(z * 768 + c * 256, 256), 256)] = wide.astype(BF)
        return 0

    lax.fori_loop(0, 2, feed, 0)
    ex.every(ex.forward, C, 2)
    lax.fori_loop(2, 4, feed, 0)
    ex.every(ex.finish, C, 2)
    for c in range(3):
        ex.shared(C, c)

    def down(y, _):
        wide = []
        for z in range(4):
            for c in range(3):
                for core in range(2):
                    parts = [ex.bufs[C][c][spot(c, core, x, y, z)] for x in range(4)]
                    wide.append(jnp.concatenate(parts, axis=0))
        here = pl.ds(pl.multiple_of(y * 256, 256), 256)
        fed = nt(hid[...], jnp.concatenate(wide, axis=1))
        out[:, here] = (res[:, here].astype(F32) + fed).astype(BF)
        return 0

    lax.fori_loop(0, 4, down, 0)
    for copy in ex.started:
        copy.wait_send()


def turn_table():
    freq = 10000.0 ** (-np.arange(32) / 32.0)
    angle = np.arange(TIMES)[:, None] * freq[None, :]
    cos = np.tile(np.cos(angle), (1, 4))
    sin = np.sin(angle)
    sin = np.tile(np.concatenate([-sin, sin], axis=1), (1, 2))
    left = np.concatenate([cos, sin], axis=1).astype(np.float32)
    terms = []
    for _ in range(3):
        term = left.astype(BF)
        terms.append(term)
        left = left - term.astype(np.float32)
    rows = np.concatenate(terms, axis=1)
    return np.concatenate([rows, np.zeros((128 - TIMES, rows.shape[1]), BF)], axis=0)


def local(
    tokens,
    norm_gain,
    qkv_weight,
    out_weight,
    variate_bias,
    ffn_weight,
    down_weight,
    sample_ids,
    variate_ids,
    time_ids,
):
    wide = jnp.pad(ffn_weight, ((0, 0), (0, 0), (0, 32)))
    turned_out = out_weight.T
    packb = jnp.concatenate(
        [
            piece
            for c in range(3)
            for piece in (
                turned_out[OUT_AT[c] : OUT_AT[c] + OUT_ROWS[c]],
                wide[0, :, c * 128 : (c + 1) * 128],
                wide[1, :, c * 128 : (c + 1) * 128],
            )
        ],
        axis=0,
    )
    tall = jnp.pad(down_weight, ((0, 32), (0, 0))).T
    packc = tall.reshape(64, 3, 128).transpose(1, 0, 2)
    slope = (variate_bias[0] - variate_bias[1]) * LOG2E
    vmem = pl.BlockSpec(memory_space=pltpu.VMEM)
    hbm = pl.BlockSpec(memory_space=pl.ANY)
    smem = pl.BlockSpec(memory_space=pltpu.SMEM)
    buffers = [
        pltpu.VMEM((128, ROWS[b][c], 128), BF) for b in (A, B, C) for c in range(3)
    ]
    return pl.pallas_call(
        kernel,
        out_shape=jax.ShapeDtypeStruct((L, D), BF),
        in_specs=[vmem, vmem, hbm, hbm, hbm, vmem, smem, vmem, vmem, vmem],
        out_specs=vmem,
        scratch_shapes=buffers
        + [
            pltpu.VMEM((L, D), BF),
            pltpu.VMEM((L, L), F32),
            pltpu.VMEM((L, L), F32),
            pltpu.VMEM((L, 128), F32),
            pltpu.VMEM((L, 128), F32),
            pltpu.VMEM((L, 128), F32),
            pltpu.VMEM((L, 128), F32),
            pltpu.VMEM((L, 256), BF),
            pltpu.VMEM((L, 256), BF),
            pltpu.VMEM((L, 256), BF),
            pltpu.VMEM((L, D), BF),
            pltpu.VMEM((L, D), BF),
            pltpu.VMEM((L, 3072), BF),
            pltpu.SemaphoreType.DMA((3, 3)),
            pltpu.SemaphoreType.DMA((3, 3, 25)),
            pltpu.SemaphoreType.DMA((3, 3, 25)),
        ],
        compiler_params=pltpu.CompilerParams(
            collective_id=0, has_side_effects=True, vmem_limit_bytes=67000000
        ),
    )(
        tokens,
        norm_gain,
        qkv_weight,
        packb,
        packc,
        jnp.asarray(turn_table()),
        slope,
        sample_ids.reshape(1, L),
        variate_ids.reshape(1, L),
        time_ids.reshape(1, L),
    )


def solution(mesh):
    return jax.shard_map(
        local,
        mesh=mesh,
        in_specs=(
            P(("dp", "mp"), None),
            P(),
            P(None, "dp", "mp"),
            P("mp", "dp"),
            P(),
            P(None, "dp", "mp"),
            P("mp", "dp"),
            P(("dp", "mp")),
            P(("dp", "mp")),
            P(("dp", "mp")),
        ),
        out_specs=P(("dp", "mp"), None),
        check_vma=False,
    )
```

```python
import jax
import jax.numpy as jnp
import numpy as np
from jax import lax
from jax.experimental import pallas as pl
from jax.experimental.pallas import tpu as pltpu
from jax.sharding import PartitionSpec as P

L = 512
D = 1024
TIMES = 32
LOG2E = 1.4426950408889634
BF = jnp.bfloat16
F32 = jnp.float32
MESH = pl.DeviceIdType.MESH

ORDERS = (("x", "y", "z"), ("y", "z", "x"), ("z", "x", "y"))
A, G1, G2, D1, D2 = range(5)
BATCHES = (
    ((("q", 0, 64),), (("k", 0, 64),), (("v", 0, 64),)),
    (
        (("o", 0, 32), ("g0", 0, 64)),
        (("o", 32, 16), ("u0", 0, 64)),
        (("o", 48, 16), ("g1", 0, 64)),
    ),
    ((("u1", 0, 64),), (("g2", 0, 64),), (("u2", 0, 64),)),
    ((("d0", 0, 48),), (("d0", 48, 16), ("d1", 0, 32)), (("d1", 32, 32),)),
    ((("d2", 0, 16),), (("d2", 16, 16),), (("d2", 32, 32),)),
)
ROWS = tuple(tuple(sum(p[2] for p in pieces) for pieces in batch) for batch in BATCHES)
HALF = tuple(tuple((r // 16 + 1) // 2 * 16 for r in rows) for rows in ROWS)
OWN = 24
NS = 25
VMEM = 58 * 2**20


def whereabouts(name):
    found = []
    for b, batch in enumerate(BATCHES):
        for c, pieces in enumerate(batch):
            row = 0
            for piece, first, count in pieces:
                if piece == name:
                    found.append((first, b, c, row, count))
                row += count
    return [part[1:] for part in sorted(found)]


class Exchange:
    def __init__(self, bufs, send, recv):
        self.bufs, self.send, self.recv = bufs, send, recv
        dp, mp = lax.axis_index("dp"), lax.axis_index("mp")
        self.pos = {"x": lax.rem(dp, 4), "y": dp // 4, "z": mp // 2}
        self.core = lax.rem(mp, 2)
        self.started = []

    def device(self, axis=None, step=0):
        pos = dict(self.pos)
        core = self.core
        if axis == "core":
            core = 1 - core
        elif axis is not None:
            pos[axis] = lax.rem(pos[axis] + step + 4, 4)
        return (pos["y"] * 4 + pos["x"], pos["z"] * 2 + core)

    def slab(self, b, c, phase, shift, half):
        a1, a2, a3 = ORDERS[c]
        at = {k: self.pos[k] for k in "xyz"}
        axis = ORDERS[c][phase]
        at[axis] = lax.rem(at[axis] + shift + 4, 4)
        buf = self.bufs[b][c]
        base = self.core * 64 + at[a3] * 16
        if phase == 0:
            first = base + at[a2] * 4 + at[a1]
            top = HALF[b][c]
            rows = pl.ds(0, top) if half == 0 else pl.ds(top, ROWS[b][c] - top)
            return buf.at[pl.ds(first, 1), rows]
        if phase == 1:
            return buf.at[pl.ds(base + at[a2] * 4 + 2 * half, 2)]
        return buf.at[pl.ds(base + 8 * half, 8)]

    def copy(self, ref, b, c, slot, device):
        return pltpu.make_async_remote_copy(
            src_ref=ref,
            dst_ref=ref,
            send_sem=self.send.at[b, c, slot],
            recv_sem=self.recv.at[b, c, slot],
            device_id=device,
            device_id_type=MESH,
        )

    def start(self, b, c, slot, ref, device):
        copy = self.copy(ref, b, c, slot, device)
        copy.start()
        self.started.append(copy)

    def first(self, b, c, p):
        axis = ORDERS[c][p]
        for slot, half, step in ((0, 0, 1), (2, 1, -1), (1, 1, 1), (3, 0, -1)):
            if self.empty(b, c, p, half):
                continue
            self.start(b, c, p * 6 + slot, self.slab(b, c, p, 0, half), self.device(axis, step))

    def empty(self, b, c, p, half):
        return p == 0 and half == 1 and HALF[b][c] == ROWS[b][c]

    def landed(self, b, c, p, slot):
        half = (0, 1, 1, 0, 0, 1)[slot]
        shift = (-1, -1, 1, 1, -2, 2)[slot]
        ref = self.slab(b, c, p, shift, half)
        self.copy(ref, b, c, p * 6 + slot, self.device(ORDERS[c][p], 1)).wait_recv()
        return ref

    def forward(self, b, c, p):
        axis = ORDERS[c][p]
        for slot, step in ((0, 1), (2, -1)):
            if self.empty(b, c, p, slot // 2):
                continue
            ref = self.landed(b, c, p, slot)
            self.start(b, c, p * 6 + 4 + slot // 2, ref, self.device(axis, step))
            if p == 2:
                self.share(b, c, slot, ref)

    def finish(self, b, c, p, slots=(1, 3, 4, 5)):
        for slot in slots:
            if self.empty(b, c, p, (0, 1, 1, 0, 0, 1)[slot]):
                continue
            ref = self.landed(b, c, p, slot)
            if p == 2:
                self.share(b, c, slot, ref)

    def share(self, b, c, slot, ref):
        self.start(b, c, 18 + slot, ref, self.device("core"))

    def plane(self, b, c, core):
        return self.bufs[b][c].at[pl.ds(core * 64 + self.pos[ORDERS[c][2]] * 16, 16)]

    def share_own(self, b, c):
        self.start(b, c, OWN, self.plane(b, c, self.core), self.device("core"))

    def shared(self, b, c):
        other = self.device("core")
        self.copy(self.plane(b, c, self.core), b, c, OWN, other).wait_recv()
        for slot in range(6):
            ref = self.slab(b, c, 2, (-1, -1, 1, 1, -2, 2)[slot], (0, 1, 1, 0, 0, 1)[slot])
            self.copy(ref, b, c, 18 + slot, other).wait_recv()

    def every(self, action, p, *batches):
        for b in batches:
            for c in range(3):
                action(b, c, p)

    def finish_some(self, b, slots):
        for c in range(3):
            self.finish(b, c, 2, slots)

    def own_planes(self, *batches):
        for b in batches:
            for c in range(3):
                self.share_own(b, c)

    def complete(self, b):
        for c in range(3):
            self.shared(b, c)


def nt(a, b):
    return lax.dot_general(a, b, (((1,), (1,)), ((), ())), preferred_element_type=F32)


def nn(a, b):
    return jnp.dot(a, b, preferred_element_type=F32)


def spot(c, core, x, y, z):
    at = {"x": x, "y": y, "z": z}
    a1, a2, a3 = ORDERS[c]
    return core * 64 + at[a3] * 16 + at[a2] * 4 + at[a1]


def normed_into(dst, src, gain, row):
    g = gain[pl.ds(row, 1), :]

    def block(i, _):
        rows = pl.ds(pl.multiple_of(i * 64, 64), 64)
        wide = src[rows, :].astype(F32)
        square = jnp.mean(wide * wide, axis=-1, keepdims=True)
        dst[rows, :] = (wide * lax.rsqrt(square + 1e-05) * g).astype(BF)
        return 0

    lax.fori_loop(0, 8, block, 0)


def kernel(
    tok_hbm, gain, qkvw, outw, ffnw, downw, table, bias, sids, vids, tids,
    out, *scratch,
):
    chunks = scratch[:15]
    (tok, xn, same, away, cq, sq, ck, sk, qs, ks, vs, att, res, hid, half, acc,
     stage, tok_sem, send, recv) = scratch[15:]
    ex = Exchange([chunks[3 * b : 3 * b + 3] for b in range(5)], send, recv)

    def tile_of(name):
        if name in "qkv":
            return qkvw.at["qkv".index(name)]
        if name == "o":
            return outw
        lanes = pl.ds(int(name[1]) * 128, 128)
        return downw.at[:, lanes] if name[0] == "d" else ffnw.at["gu".index(name[0]), :, lanes]

    def owns(b):
        copies = []
        for c, pieces in enumerate(BATCHES[b]):
            at = ex.bufs[b][c].at[spot(c, ex.core, ex.pos["x"], ex.pos["y"], ex.pos["z"])]
            row = 0
            for k, (name, first, count) in enumerate(pieces):
                copies.append(
                    pltpu.make_async_copy(
                        tile_of(name).at[pl.ds(first, count)],
                        at.at[pl.ds(row, count)],
                        stage.at[b, c, k],
                    )
                )
                row += count
        return copies

    for b in range(5):
        for copy in owns(b):
            copy.start()
    fetch = pltpu.make_async_copy(tok_hbm, tok, tok_sem)
    fetch.start()
    barrier = pltpu.get_barrier_semaphore()
    for axis in "xyz":
        for step in (1, -1):
            pl.semaphore_signal(barrier, inc=1, device_id=ex.device(axis, step), device_id_type=MESH)
    pl.semaphore_signal(barrier, inc=1, device_id=ex.device("core"), device_id_type=MESH)
    pl.semaphore_wait(barrier, 7)

    for b in range(5):
        for copy in owns(b):
            copy.wait()
        ex.every(ex.first, 0, b)

    eye = (
        lax.broadcasted_iota(jnp.int32, (L, L), 0) == lax.broadcasted_iota(jnp.int32, (L, L), 1)
    ).astype(F32).astype(BF)

    def column(ids):
        row = jnp.broadcast_to(ids[...].astype(F32), (128, L)).astype(BF)
        return nt(eye, row)

    def matches(ids):
        col = column(ids)
        row = jnp.broadcast_to(ids[...].astype(F32), (L, L))
        return jnp.concatenate([col] * 4, axis=1) == row

    same[...] = jnp.where(matches(vids), 1.0, 0.0)
    away[...] = jnp.where(matches(sids), 0.0, -1e30)

    ex.every(ex.forward, 0, A, G1, G2, D1, D2)
    fetch.wait()
    normed_into(xn, tok, gain, 0)
    for b in (A, G1, G2):
        ex.every(ex.finish, 0, b)
        ex.every(ex.first, 1, b)
    ex.every(ex.finish, 0, D1, D2)

    lanes = lax.broadcasted_iota(jnp.int32, (L, 128), 1).astype(F32)
    hot = jnp.where(column(tids) == lanes, 1.0, 0.0).astype(BF)
    turn = nn(hot, table[...])
    cos = turn[:, 0:128] + turn[:, 256:384] + turn[:, 512:640]
    sin = turn[:, 128:256] + turn[:, 384:512] + turn[:, 640:768]
    cq[...] = cos * (LOG2E / 8.0)
    sq[...] = sin * (LOG2E / 8.0)
    ck[...] = cos
    sk[...] = sin

    ex.every(ex.forward, 1, A)
    ex.every(ex.first, 1, D1, D2)
    ex.every(ex.forward, 1, G1)
    ex.every(ex.finish, 1, A)
    ex.every(ex.first, 2, A)
    ex.own_planes(A)
    ex.every(ex.forward, 1, G2, D1, D2)
    ex.every(ex.finish, 1, G1)
    ex.own_planes(G1)
    ex.every(ex.forward, 2, A)
    ex.every(ex.first, 2, G1)
    ex.finish_some(A, (1, 3))
    ex.every(ex.finish, 1, G2, D1, D2)
    ex.finish_some(A, (4, 5))
    ex.own_planes(G2, D1, D2)
    ex.complete(A)

    def columns(name, z):
        sides = []
        for core in range(2):
            parts = [
                ex.bufs[b][c][spot(c, core, x, y, z), pl.ds(row, count), :]
                for y in range(4)
                for x in range(4)
                for b, c, row, count in whereabouts(name)
            ]
            sides.append(jnp.concatenate(parts, axis=0))
        return jnp.concatenate(sides, axis=1)

    def outputs(names, y):
        wide = []
        for z in range(4):
            for name in names:
                for core in range(2):
                    parts = [
                        ex.bufs[b][c][spot(c, core, x, y, z), pl.ds(row, count), :]
                        for x in range(4)
                        for b, c, row, count in whereabouts(name)
                    ]
                    wide.append(jnp.concatenate(parts, axis=0))
        return jnp.concatenate(wide, axis=1)

    def turned(raw, cosine, sine):
        lane = lax.rem(lax.broadcasted_iota(jnp.int32, (L, 128), 1), 64)
        done = []
        for t in range(2):
            v = raw[:, t * 128 : (t + 1) * 128]
            other = jnp.where(lane < 32, pltpu.roll(v, 96, 1), pltpu.roll(v, 32, 1))
            done.append(v * cosine[...] + other * sine[...])
        return jnp.concatenate(done, axis=1).astype(BF)

    def group(z):
        qs[...] = turned(nn(xn[...], columns("q", z)), cq, sq)
        ks[...] = turned(nn(xn[...], columns("k", z)), ck, sk)
        vs[...] = nn(xn[...], columns("v", z)).astype(BF)

        def head(h):
            mine = lax.broadcasted_iota(jnp.int32, (L, 256), 1) // 64 == h
            q = jnp.where(mine, qs[...], jnp.zeros((), BF))
            s = nt(q, ks[...]) + same[...] * ((bias[0, z * 4 + h] - bias[1, z * 4 + h]) * LOG2E) + away[...]
            e = jnp.exp2(s - jnp.max(s, axis=1, keepdims=True))
            total = jnp.sum(e, axis=1, keepdims=True)
            got = (nn(e.astype(BF), vs[...]) * (1.0 / total)).astype(BF)
            here = pl.ds(z * 256, 256)
            att[:, here] = jnp.where(mine, got, att[:, here])

        for h in range(4):
            head(h)

    att[...] = jnp.zeros_like(att)
    group(0)
    ex.every(ex.forward, 2, G1)
    ex.every(ex.first, 2, G2)
    group(1)
    group(2)
    ex.finish_some(G1, (1, 3))
    group(3)
    ex.finish_some(G1, (4, 5))
    ex.every(ex.forward, 2, G2)
    ex.every(ex.first, 2, D1, D2)
    ex.complete(G1)

    def here(y):
        return pl.ds(pl.multiple_of(y * 256, 256), 256)

    def project(y, _):
        mixed = nt(att[...], outputs(("o",), y))
        res[:, here(y)] = (tok[:, here(y)].astype(F32) + mixed).astype(BF)
        return 0

    lax.fori_loop(0, 4, project, 0)
    normed_into(xn, res, gain, 1)

    def soft(gate):
        return gate / (1.0 + jnp.exp(-gate))

    def feed(k, gate, up):
        def step(z, _):
            bent = half[:, here(z)] if gate is None else soft(nn(xn[...], columns(gate, z)))
            hidden = bent * nn(xn[...], columns(up, z))
            hid[:, pl.ds(pl.multiple_of(k * 1024 + z * 256, 256), 256)] = hidden.astype(BF)
            return 0

        lax.fori_loop(0, 4, step, 0)

    def gates(z, _):
        half[:, here(z)] = soft(nn(xn[...], columns("g1", z)))
        return 0

    feed(0, "g0", "u0")
    ex.finish_some(G2, (1, 3, 4, 5))
    lax.fori_loop(0, 4, gates, 0)
    ex.every(ex.forward, 2, D1, D2)
    ex.complete(G2)
    feed(1, None, "u1")
    ex.finish_some(D1, (1, 3))
    feed(2, "g2", "u2")
    ex.finish_some(D1, (4, 5))
    ex.every(ex.finish, 2, D2)
    ex.complete(D1)

    def down_first(y, _):
        at = pl.ds(0, 2048)
        wide = [outputs((name,), y) for name in ("d0", "d1")]
        acc[:, here(y)] = res[:, here(y)].astype(F32) + nt(
            hid[:, at], jnp.concatenate(wide, axis=1)
        )
        return 0

    def down_last(y, _):
        fed = nt(hid[:, pl.ds(2048, 1024)], outputs(("d2",), y))
        out[:, here(y)] = (acc[:, here(y)] + fed).astype(BF)
        return 0

    lax.fori_loop(0, 4, down_first, 0)
    ex.complete(D2)
    lax.fori_loop(0, 4, down_last, 0)
    for copy in ex.started:
        copy.wait_send()


def turn_table():
    freq = 10000.0 ** (-np.arange(32) / 32.0)
    angle = np.arange(TIMES)[:, None] * freq[None, :]
    cos = np.tile(np.cos(angle), (1, 4))
    sin = np.sin(angle)
    sin = np.tile(np.concatenate([-sin, sin], axis=1), (1, 2))
    left = np.concatenate([cos, sin], axis=1).astype(np.float32)
    terms = []
    for _ in range(3):
        term = left.astype(BF)
        terms.append(term)
        left = left - term.astype(np.float32)
    rows = np.concatenate(terms, axis=1)
    return np.concatenate([rows, np.zeros((128 - TIMES, rows.shape[1]), BF)], axis=0)


def local(
    tokens,
    norm_gain,
    qkv_weight,
    out_weight,
    variate_bias,
    ffn_weight,
    down_weight,
    sample_ids,
    variate_ids,
    time_ids,
):
    ffn_wide = jnp.pad(ffn_weight, ((0, 0), (0, 0), (0, 32)))
    down_wide = jnp.pad(down_weight.T, ((0, 0), (0, 32)))
    vmem = pl.BlockSpec(memory_space=pltpu.VMEM)
    hbm = pl.BlockSpec(memory_space=pl.ANY)
    smem = pl.BlockSpec(memory_space=pltpu.SMEM)
    buffers = [
        pltpu.VMEM((128, ROWS[b][c], 128), BF) for b in range(5) for c in range(3)
    ]
    return pl.pallas_call(
        kernel,
        out_shape=jax.ShapeDtypeStruct((L, D), BF),
        in_specs=[hbm, vmem, hbm, hbm, hbm, hbm, vmem, smem, vmem, vmem, vmem],
        out_specs=vmem,
        scratch_shapes=buffers
        + [
            pltpu.VMEM((L, D), BF),
            pltpu.VMEM((L, D), BF),
            pltpu.VMEM((L, L), F32),
            pltpu.VMEM((L, L), F32),
            pltpu.VMEM((L, 128), F32),
            pltpu.VMEM((L, 128), F32),
            pltpu.VMEM((L, 128), F32),
            pltpu.VMEM((L, 128), F32),
            pltpu.VMEM((L, 256), BF),
            pltpu.VMEM((L, 256), BF),
            pltpu.VMEM((L, 256), BF),
            pltpu.VMEM((L, D), BF),
            pltpu.VMEM((L, D), BF),
            pltpu.VMEM((L, 3072), BF),
            pltpu.VMEM((L, D), F32),
            pltpu.VMEM((L, D), F32),
            pltpu.SemaphoreType.DMA((5, 3, 2)),
            pltpu.SemaphoreType.DMA,
            pltpu.SemaphoreType.DMA((5, 3, NS)),
            pltpu.SemaphoreType.DMA((5, 3, NS)),
        ],
        compiler_params=pltpu.CompilerParams(
            collective_id=0, has_side_effects=True, vmem_limit_bytes=VMEM
        ),
    )(
        tokens,
        norm_gain,
        qkv_weight,
        out_weight.T,
        ffn_wide,
        down_wide,
        jnp.asarray(turn_table()),
        variate_bias,
        sample_ids.reshape(1, L),
        variate_ids.reshape(1, L),
        time_ids.reshape(1, L),
    )


def solution(mesh):
    return jax.shard_map(
        local,
        mesh=mesh,
        in_specs=(
            P(("dp", "mp"), None),
            P(),
            P(None, "dp", "mp"),
            P("mp", "dp"),
            P(),
            P(None, "dp", "mp"),
            P("mp", "dp"),
            P(("dp", "mp")),
            P(("dp", "mp")),
            P(("dp", "mp")),
        ),
        out_specs=P(("dp", "mp"), None),
        check_vma=False,
    )
```

```python
import jax
import jax.numpy as jnp
import numpy as np
from jax import lax
from jax.experimental import pallas as pl
from jax.experimental.pallas import tpu as pltpu
from jax.sharding import PartitionSpec as P

L = 512
D = 1024
TIMES = 32
LOG2E = 1.4426950408889634
BF = jnp.bfloat16
F32 = jnp.float32
MESH = pl.DeviceIdType.MESH

ORDERS = (("x", "y", "z"), ("y", "z", "x"), ("z", "x", "y"))
A, G1, G2, D1, D2 = range(5)
BATCHES = (
    ((("q", 0, 64),), (("k", 0, 64),), (("v", 0, 64),)),
    (
        (("o", 0, 32), ("g0", 0, 64)),
        (("o", 32, 16), ("u0", 0, 64)),
        (("o", 48, 16), ("g1", 0, 64)),
    ),
    ((("u1", 0, 64),), (("g2", 0, 64),), (("u2", 0, 64),)),
    ((("d0", 0, 48),), (("d0", 48, 16), ("d1", 0, 32)), (("d1", 32, 32),)),
    ((("d2", 0, 16),), (("d2", 16, 16),), (("d2", 32, 32),)),
)
ROWS = tuple(tuple(sum(p[2] for p in pieces) for pieces in batch) for batch in BATCHES)
START = tuple(tuple(sum(ROWS[k][c] for k in range(b)) for c in range(3)) for b in range(6))
GROUPS = (
    ((A, G1), (G1, D2 + 1)),
    ((A, G1), (G1, G2), (G2, D2 + 1)),
    tuple((b, b + 1) for b in range(5)),
)
FIRST_SEM = (0, 36, 90, 180, 270)
SEMS = 276
HALF_OF = (0, 1, 1, 0, 0, 1)
SHIFT_OF = (-1, -1, 1, 1, -2, 2)
VMEM = 58 * 2**20


def whereabouts(name):
    found = []
    for b, batch in enumerate(BATCHES):
        for c, pieces in enumerate(batch):
            row = 0
            for piece, first, count in pieces:
                if piece == name:
                    found.append((first, c, START[b][c] + row, count))
                row += count
    return [part[1:] for part in sorted(found)]


class Exchange:
    def __init__(self, bufs, send, recv):
        self.bufs, self.send, self.recv = bufs, send, recv
        dp, mp = lax.axis_index("dp"), lax.axis_index("mp")
        self.pos = {"x": lax.rem(dp, 4), "y": dp // 4, "z": mp // 2}
        self.core = lax.rem(mp, 2)
        self.started = []

    def device(self, axis=None, step=0):
        pos = dict(self.pos)
        core = self.core
        if axis == "core":
            core = 1 - core
        elif axis is not None:
            pos[axis] = lax.rem(pos[axis] + step + 4, 4)
        return (pos["y"] * 4 + pos["x"], pos["z"] * 2 + core)

    def span(self, p, g, c):
        first, last = GROUPS[p][g]
        return START[first][c], START[last][c]

    def slab(self, p, g, c, shift, half):
        a1, a2, a3 = ORDERS[c]
        at = {k: self.pos[k] for k in "xyz"}
        axis = ORDERS[c][p]
        at[axis] = lax.rem(at[axis] + shift + 4, 4)
        low, high = self.span(p, g, c)
        base = self.core * 64 + at[a3] * 16
        count = (1, 4, 16)[p]
        if p < 2:
            base = base + at[a2] * 4
        if p < 1:
            base = base + at[a1]
        if half is not None and p == 0:
            middle = low + ((high - low) // 16 + 1) // 2 * 16
            low, high = ((low, middle), (middle, high))[half]
        elif half is not None:
            count = count // 2
            base = base + half * count
        return self.bufs[c].at[pl.ds(base, count), pl.ds(low, high - low)]

    def copy(self, ref, sem, device):
        return pltpu.make_async_remote_copy(
            src_ref=ref,
            dst_ref=ref,
            send_sem=self.send.at[sem],
            recv_sem=self.recv.at[sem],
            device_id=device,
            device_id_type=MESH,
        )

    def start(self, ref, sem, device):
        copy = self.copy(ref, sem, device)
        copy.start()
        self.started.append(copy)

    def sem(self, p, g, c, slot):
        return FIRST_SEM[p] + (g * 3 + c) * 6 + slot

    def first(self, p, g):
        for c in range(3):
            axis = ORDERS[c][p]
            for slot, step in ((0, 1), (2, -1), (1, 1), (3, -1)):
                if p == 0 and slot % 2:
                    continue
                half = None if p == 0 else HALF_OF[slot]
                self.start(
                    self.slab(p, g, c, 0, half), self.sem(p, g, c, slot), self.device(axis, step)
                )

    def landed(self, p, g, c, slot):
        half = None if p == 0 and slot < 4 else HALF_OF[slot]
        ref = self.slab(p, g, c, SHIFT_OF[slot], half)
        self.copy(ref, self.sem(p, g, c, slot), self.device(ORDERS[c][p], 1)).wait_recv()
        return ref

    def forward(self, p, g):
        for c in range(3):
            axis = ORDERS[c][p]
            for slot, step in ((0, 1), (2, -1)):
                self.landed(p, g, c, slot)
                ref = self.slab(p, g, c, SHIFT_OF[slot], HALF_OF[slot])
                self.start(ref, self.sem(p, g, c, 4 + slot // 2), self.device(axis, step))
                if p == 2:
                    self.share(g, c, slot, ref)

    def finish(self, p, g, slots=(1, 3, 4, 5)):
        for c in range(3):
            for slot in slots:
                if p == 0 and slot < 4:
                    continue
                ref = self.landed(p, g, c, slot)
                if p == 2:
                    self.share(g, c, slot, ref)

    def share(self, g, c, slot, ref):
        self.start(ref, self.sem(3, g, c, slot), self.device("core"))

    def plane(self, k, c):
        low, high = self.span(0, k, c)
        first = self.core * 64 + self.pos[ORDERS[c][2]] * 16
        return self.bufs[c].at[pl.ds(first, 16), pl.ds(low, high - low)]

    def share_own(self, k):
        for c in range(3):
            self.start(self.plane(k, c), FIRST_SEM[4] + k * 3 + c, self.device("core"))

    def complete(self, g):
        other = self.device("core")
        for c in range(3):
            if g < 2:
                self.copy(self.plane(g, c), FIRST_SEM[4] + g * 3 + c, other).wait_recv()
            for slot in range(6):
                ref = self.slab(2, g, c, SHIFT_OF[slot], HALF_OF[slot])
                self.copy(ref, self.sem(3, g, c, slot), other).wait_recv()


def nt(a, b):
    return lax.dot_general(a, b, (((1,), (1,)), ((), ())), preferred_element_type=F32)


def nn(a, b):
    return jnp.dot(a, b, preferred_element_type=F32)


def spot(c, core, x, y, z):
    at = {"x": x, "y": y, "z": z}
    a1, a2, a3 = ORDERS[c]
    return core * 64 + at[a3] * 16 + at[a2] * 4 + at[a1]


def normed_into(dst, src, gain, row):
    g = gain[pl.ds(row, 1), :]

    def block(i, _):
        rows = pl.ds(pl.multiple_of(i * 64, 64), 64)
        wide = src[rows, :].astype(F32)
        square = jnp.mean(wide * wide, axis=-1, keepdims=True)
        dst[rows, :] = (wide * lax.rsqrt(square + 1e-05) * g).astype(BF)
        return 0

    lax.fori_loop(0, 8, block, 0)


def kernel(
    tok_hbm, gain, qkvw, outw, wide, table, bias, sids, vids, tids,
    out, *scratch,
):
    (tok, xn, same, away, cq, sq, ck, sk, qs, ks, vs, att, res, hid, half, acc,
     stage, tok_sem, send, recv) = scratch[3:]
    ex = Exchange(scratch[:3], send, recv)

    def tile_of(name):
        if name in "qkv":
            return qkvw.at["qkv".index(name)]
        if name == "o":
            return outw
        lanes = pl.ds(int(name[1]) * 128, 128)
        return wide.at["gud".index(name[0]), :, lanes]

    def owns(b):
        copies = []
        for c, pieces in enumerate(BATCHES[b]):
            at = ex.bufs[c].at[spot(c, ex.core, ex.pos["x"], ex.pos["y"], ex.pos["z"])]
            row = START[b][c]
            for k, (name, first, count) in enumerate(pieces):
                copies.append(
                    pltpu.make_async_copy(
                        tile_of(name).at[pl.ds(first, count)],
                        at.at[pl.ds(row, count)],
                        stage.at[b, c, k],
                    )
                )
                row += count
        return copies

    for b in range(5):
        for copy in owns(b):
            copy.start()
    fetch = pltpu.make_async_copy(tok_hbm, tok, tok_sem)
    fetch.start()
    barrier = pltpu.get_barrier_semaphore()
    for axis in "xyz":
        for step in (1, -1):
            pl.semaphore_signal(barrier, inc=1, device_id=ex.device(axis, step), device_id_type=MESH)
    pl.semaphore_signal(barrier, inc=1, device_id=ex.device("core"), device_id_type=MESH)
    pl.semaphore_wait(barrier, 7)

    for k in range(2):
        for b in range(*GROUPS[0][k]):
            for copy in owns(b):
                copy.wait()
        ex.first(0, k)

    eye = (
        lax.broadcasted_iota(jnp.int32, (L, L), 0) == lax.broadcasted_iota(jnp.int32, (L, L), 1)
    ).astype(F32).astype(BF)

    def column(ids):
        row = jnp.broadcast_to(ids[...].astype(F32), (128, L)).astype(BF)
        return nt(eye, row)

    def matches(ids):
        col = column(ids)
        row = jnp.broadcast_to(ids[...].astype(F32), (L, L))
        return jnp.concatenate([col] * 4, axis=1) == row

    same[...] = jnp.where(matches(vids), 1.0, 0.0)
    away[...] = jnp.where(matches(sids), 0.0, -1e30)

    ex.forward(0, 0)
    ex.forward(0, 1)
    fetch.wait()
    normed_into(xn, tok, gain, 0)
    for k in range(2):
        ex.finish(0, k)
        ex.first(1, k)

    lanes = lax.broadcasted_iota(jnp.int32, (L, 128), 1).astype(F32)
    hot = jnp.where(column(tids) == lanes, 1.0, 0.0).astype(BF)
    turn = nn(hot, table[...])
    cos = turn[:, 0:128] + turn[:, 256:384] + turn[:, 512:640]
    sin = turn[:, 128:256] + turn[:, 384:512] + turn[:, 640:768]
    cq[...] = cos * (LOG2E / 8.0)
    sq[...] = sin * (LOG2E / 8.0)
    ck[...] = cos
    sk[...] = sin

    ex.forward(1, 0)
    ex.first(1, 2)
    ex.forward(1, 1)
    ex.finish(1, 0)
    ex.first(2, A)
    ex.share_own(0)
    ex.forward(1, 2)
    ex.finish(1, 1)
    ex.forward(2, A)
    ex.first(2, G1)
    ex.finish(2, A, (1, 3))
    ex.finish(1, 2)
    ex.finish(2, A, (4, 5))
    ex.share_own(1)
    ex.complete(A)

    def columns(name, z):
        sides = []
        for core in range(2):
            parts = [
                ex.bufs[c][spot(c, core, x, y, z), pl.ds(row, count), :]
                for y in range(4)
                for x in range(4)
                for c, row, count in whereabouts(name)
            ]
            sides.append(jnp.concatenate(parts, axis=0))
        return jnp.concatenate(sides, axis=1)

    def outputs(names, y):
        wide = []
        for z in range(4):
            for name in names:
                for core in range(2):
                    parts = [
                        ex.bufs[c][spot(c, core, x, y, z), pl.ds(row, count), :]
                        for x in range(4)
                        for c, row, count in whereabouts(name)
                    ]
                    wide.append(jnp.concatenate(parts, axis=0))
        return jnp.concatenate(wide, axis=1)

    def turned(raw, cosine, sine):
        lane = lax.rem(lax.broadcasted_iota(jnp.int32, (L, 128), 1), 64)
        done = []
        for t in range(2):
            v = raw[:, t * 128 : (t + 1) * 128]
            other = jnp.where(lane < 32, pltpu.roll(v, 96, 1), pltpu.roll(v, 32, 1))
            done.append(v * cosine[...] + other * sine[...])
        return jnp.concatenate(done, axis=1).astype(BF)

    def group(z, between=None, at=0):
        qs[...] = turned(nn(xn[...], columns("q", z)), cq, sq)
        ks[...] = turned(nn(xn[...], columns("k", z)), ck, sk)
        vs[...] = nn(xn[...], columns("v", z)).astype(BF)

        def head(h):
            mine = lax.broadcasted_iota(jnp.int32, (L, 256), 1) // 64 == h
            q = jnp.where(mine, qs[...], jnp.zeros((), BF))
            s = nt(q, ks[...]) + same[...] * ((bias[0, z * 4 + h] - bias[1, z * 4 + h]) * LOG2E) + away[...]
            e = jnp.exp2(s - jnp.max(s, axis=1, keepdims=True))
            total = jnp.sum(e, axis=1, keepdims=True)
            got = (nn(e.astype(BF), vs[...]) * (1.0 / total)).astype(BF)
            here = pl.ds(z * 256, 256)
            att[:, here] = jnp.where(mine, got, att[:, here])

        for h in range(4):
            if between is not None and h == at:
                between()
            head(h)

    att[...] = jnp.zeros_like(att)
    group(0, lambda: (ex.forward(2, G1), ex.first(2, G2)))
    group(1)
    ex.finish(2, G1, (1, 3))
    group(2)
    ex.finish(2, G1, (4, 5))
    group(3, lambda: (ex.forward(2, G2), ex.first(2, D1), ex.first(2, D2)), 2)
    ex.complete(G1)

    def here(y):
        return pl.ds(pl.multiple_of(y * 256, 256), 256)

    def project(y, _):
        mixed = nt(att[...], outputs(("o",), y))
        res[:, here(y)] = (tok[:, here(y)].astype(F32) + mixed).astype(BF)
        return 0

    lax.fori_loop(0, 4, project, 0)
    normed_into(xn, res, gain, 1)

    def soft(gate):
        return gate / (1.0 + jnp.exp(-gate))

    def feed(k, gate, up):
        def step(z, _):
            bent = half[:, here(z)] if gate is None else soft(nn(xn[...], columns(gate, z)))
            hidden = bent * nn(xn[...], columns(up, z))
            hid[:, pl.ds(pl.multiple_of(k * 1024 + z * 256, 256), 256)] = hidden.astype(BF)
            return 0

        lax.fori_loop(0, 4, step, 0)

    def gates(z, _):
        half[:, here(z)] = soft(nn(xn[...], columns("g1", z)))
        return 0

    feed(0, "g0", "u0")
    ex.finish(2, G2)
    ex.forward(2, D1)
    lax.fori_loop(0, 4, gates, 0)
    ex.complete(G2)
    ex.forward(2, D2)
    feed(1, None, "u1")
    ex.finish(2, D1)
    feed(2, "g2", "u2")
    ex.finish(2, D2)
    ex.complete(D1)

    def down_first(y, _):
        at = pl.ds(0, 2048)
        wide = [outputs((name,), y) for name in ("d0", "d1")]
        acc[:, here(y)] = res[:, here(y)].astype(F32) + nt(
            hid[:, at], jnp.concatenate(wide, axis=1)
        )
        return 0

    def down_last(y, _):
        fed = nt(hid[:, pl.ds(2048, 1024)], outputs(("d2",), y))
        out[:, here(y)] = (acc[:, here(y)] + fed).astype(BF)
        return 0

    lax.fori_loop(0, 4, down_first, 0)
    ex.complete(D2)
    lax.fori_loop(0, 4, down_last, 0)
    for copy in ex.started:
        copy.wait_send()


def turn_table():
    freq = 10000.0 ** (-np.arange(32) / 32.0)
    angle = np.arange(TIMES)[:, None] * freq[None, :]
    cos = np.tile(np.cos(angle), (1, 4))
    sin = np.sin(angle)
    sin = np.tile(np.concatenate([-sin, sin], axis=1), (1, 2))
    left = np.concatenate([cos, sin], axis=1).astype(np.float32)
    terms = []
    for _ in range(3):
        term = left.astype(BF)
        terms.append(term)
        left = left - term.astype(np.float32)
    rows = np.concatenate(terms, axis=1)
    return np.concatenate([rows, np.zeros((128 - TIMES, rows.shape[1]), BF)], axis=0)


def local(
    tokens,
    norm_gain,
    qkv_weight,
    out_weight,
    variate_bias,
    ffn_weight,
    down_weight,
    sample_ids,
    variate_ids,
    time_ids,
):
    wide = jnp.pad(ffn_weight, ((0, 1), (0, 0), (0, 32))) + jnp.pad(
        down_weight.T[None], ((2, 0), (0, 0), (0, 32))
    )
    vmem = pl.BlockSpec(memory_space=pltpu.VMEM)
    hbm = pl.BlockSpec(memory_space=pl.ANY)
    smem = pl.BlockSpec(memory_space=pltpu.SMEM)
    buffers = [
        pltpu.VMEM((128, START[5][c], 128), BF) for c in range(3)
    ]
    return pl.pallas_call(
        kernel,
        out_shape=pltpu.VMEM((L, D), BF),
        in_specs=[hbm, vmem, hbm, hbm, hbm, vmem, smem, vmem, vmem, vmem],
        out_specs=vmem,
        scratch_shapes=buffers
        + [
            pltpu.VMEM((L, D), BF),
            pltpu.VMEM((L, D), BF),
            pltpu.VMEM((L, L), F32),
            pltpu.VMEM((L, L), F32),
            pltpu.VMEM((L, 128), F32),
            pltpu.VMEM((L, 128), F32),
            pltpu.VMEM((L, 128), F32),
            pltpu.VMEM((L, 128), F32),
            pltpu.VMEM((L, 256), BF),
            pltpu.VMEM((L, 256), BF),
            pltpu.VMEM((L, 256), BF),
            pltpu.VMEM((L, D), BF),
            pltpu.VMEM((L, D), BF),
            pltpu.VMEM((L, 3072), BF),
            pltpu.VMEM((L, D), F32),
            pltpu.VMEM((L, D), F32),
            pltpu.SemaphoreType.DMA((5, 3, 2)),
            pltpu.SemaphoreType.DMA,
            pltpu.SemaphoreType.DMA((SEMS,)),
            pltpu.SemaphoreType.DMA((SEMS,)),
        ],
        compiler_params=pltpu.CompilerParams(
            collective_id=0, has_side_effects=True, vmem_limit_bytes=VMEM
        ),
    )(
        tokens,
        norm_gain,
        qkv_weight,
        out_weight.T,
        wide,
        jnp.asarray(turn_table()),
        variate_bias,
        sample_ids.reshape(1, L),
        variate_ids.reshape(1, L),
        time_ids.reshape(1, L),
    )


def solution(mesh):
    return jax.shard_map(
        local,
        mesh=mesh,
        in_specs=(
            P(("dp", "mp"), None),
            P(),
            P(None, "dp", "mp"),
            P("mp", "dp"),
            P(),
            P(None, "dp", "mp"),
            P("mp", "dp"),
            P(("dp", "mp")),
            P(("dp", "mp")),
            P(("dp", "mp")),
        ),
        out_specs=P(("dp", "mp"), None),
        check_vma=False,
    )
```
